32 devices in a mesh: win: 4 (over x, core), lat: 8 (over z, y).
Axes of the slice: x: 2, y: 2, z: 4, core: 2. Of those that a mesh axis runs over, the one named last changes fastest.
Arguments:
- perturbation: float32 [4, 64, 20, 768], P('win', 'lat'), may hold values from -6 to 6
- lat_offset: int32 [4, 64, 20, 768], P('win', 'lat'), may hold values from -1 to 0
- lon_offset: int32 [4, 64, 20, 768], P('win', 'lat'), may hold values from -4 to 3
- lat_weight: float32 [4, 64, 20, 768], P('win', 'lat'), may hold values from 0 to 0.3
- lon_weight: float32 [4, 64, 20, 768], P('win', 'lat'), may hold values from 0 to 0.3
- spectral_var: float32 [64, 768], P(None, 'lat'), may hold values from 0.5 to 4
Outputs:
- weighted_error: float32 [4, 64, 20, 768], P('win', 'lat')
The draws below stay inside these ranges and needn't reach their ends.
All inputs are finite; a program needn't handle non-finite values.
Results may differ from the reference program's by a relative error of at most 0.0003.
Values sent between devices are 32-bit elements; how exact they have to be, the bound alone decides.
No kernel may reach another device: no remote copies, remote signals or barrier semaphores. Data moves between devices by JAX's collectives and lax.ppermute only.
A program may use at most 64 MiB of HBM per device.

```python
import math
import jax
import jax.numpy as jnp
from jax import lax

NLON = 768
LEVELS = 20
STEPS = 4
LON_REACH = 4
NLAT = 64
MM = 384
NWIN = 4


def touch_ends(array, rng, smallest, top_value):
    longest = array.shape.index(max(array.shape))
    spots = []
    for shift in (0, 1):
        where = [jax.random.randint(jax.random.fold_in(rng, axis), (), 0, length) for axis, length in enumerate(array.shape)]
        where[longest] = (where[longest] + shift) % array.shape[longest]
        spots.append(tuple(where))
    return array.at[spots[0]].set(smallest).at[spots[1]].set(top_value)


def steps_of(rng, dims, split, smallest, largest):
    factor_of, own = 1.0, jax.random.fold_in(rng, 6)
    for axis_at, blocks in split:
        steps = jnp.exp(jax.random.uniform(jax.random.fold_in(own, axis_at), (blocks,), jnp.float32, smallest / len(split), largest / len(split)))
        factor_of = factor_of * jnp.repeat(steps, dims[axis_at] // blocks).reshape([-1 if axis == axis_at else 1 for axis in range(len(dims))])
    return factor_of


def scatter_about(own_key, dims, spread, bound, split=(), kind=jnp.bfloat16):
    factor_of = steps_of(own_key, dims, split, -0.22, 0.18) if split else 1.0
    values = jax.random.normal(own_key, dims, jnp.float32) * spread * factor_of
    return jnp.minimum(jnp.maximum(values, -bound), bound).astype(kind)


def setup_inputs(seed: int = 0) -> dict:
    splits = jax.random.split(jax.random.key(seed), 7)
    return {
        "perturbation": scatter_about(splits[0], (NWIN, NLAT, LEVELS, NLON), 1.0, 6.0, ((0, 4), (1, 8)), jnp.float32),
        "lat_offset": touch_ends(jax.random.randint(splits[1], (NWIN, NLAT, LEVELS, NLON), -1, 1), jax.random.fold_in(splits[1], 1), -1, 0).astype(jnp.int32),
        "lon_offset": touch_ends(jax.random.randint(splits[2], (NWIN, NLAT, LEVELS, NLON), -LON_REACH, LON_REACH), jax.random.fold_in(splits[2], 1), -LON_REACH, LON_REACH - 1).astype(jnp.int32),
        "lat_weight": jnp.clip(0.3 * jax.random.uniform(splits[3], (NWIN, NLAT, LEVELS, NLON), jnp.float32) ** steps_of(splits[3], (NWIN, NLAT, LEVELS, NLON), ((0, 4), (1, 8)), -0.2, 0.2), 0.0, 0.3),
        "lon_weight": jnp.clip(0.3 * jax.random.uniform(splits[4], (NWIN, NLAT, LEVELS, NLON), jnp.float32) ** steps_of(splits[4], (NWIN, NLAT, LEVELS, NLON), ((0, 4), (1, 8)), -0.2, 0.2), 0.0, 0.3),
        "spectral_var": jnp.clip(jnp.exp(math.log(4.0) - 2.0794415 * jax.random.uniform(splits[5], (NLAT, 2 * MM), jnp.float32) ** steps_of(splits[5], (NLAT, 2 * MM), ((1, 8),), -0.2, 0.2)), 0.5, 4.0),
    }


def interpolate(padded, lat_offset, lon_offset, lat_weight, lon_weight):
    row_count, level_count, lon_count = lat_offset.shape
    flattened = padded.reshape(-1)
    row_index = jnp.arange(row_count, dtype=jnp.int32)[:, None, None] + 1 + lat_offset
    level_index = jnp.arange(level_count, dtype=jnp.int32)[None, :, None]
    column = jnp.arange(lon_count, dtype=jnp.int32)[None, None, :] + lon_offset
    west_index = column % lon_count
    east_index = (column + 1) % lon_count
    lower_base = (row_index * level_count + level_index) * lon_count
    upper_base = lower_base + level_count * lon_count
    lower_west = jnp.take(flattened, lower_base + west_index)
    lower_east = jnp.take(flattened, lower_base + east_index)
    upper_west = jnp.take(flattened, upper_base + west_index)
    upper_east = jnp.take(flattened, upper_base + east_index)
    mixed_lower = (1.0 - lon_weight) * lower_west + lon_weight * lower_east
    mixed_upper = (1.0 - lon_weight) * upper_west + lon_weight * upper_east
    return (1.0 - lat_weight) * mixed_lower + lat_weight * mixed_upper

def lat_table(lat_count):
    orders = jnp.arange(lat_count, dtype=jnp.int32)[:, None]
    points = jnp.arange(lat_count, dtype=jnp.int32)[None, :]
    angles = ((2 * points + 1) * orders % (4 * lat_count)).astype(jnp.float32) * (math.pi / (2 * lat_count))
    scaling = jnp.where(orders == 0, math.sqrt(1.0 / lat_count), math.sqrt(2.0 / lat_count)).astype(jnp.float32)
    return scaling * jnp.cos(angles)

def propagate(window_args):
    initial, lat_offset, lon_offset, lat_weight, lon_weight = window_args
    current = initial
    for _ in range(STEPS):
        padded = jnp.pad(current, ((1, 1), (0, 0), (0, 0)))
        current = interpolate(padded, lat_offset, lon_offset, lat_weight, lon_weight)
    return current

def reference(perturbation, lat_offset, lon_offset, lat_weight, lon_weight, spectral_var):
    carried = lax.map(propagate, (perturbation, lat_offset, lon_offset, lat_weight, lon_weight))
    previous = jnp.concatenate([jnp.zeros_like(carried[:1]), carried[:-1]], axis=0)
    model_error = perturbation - previous
    half_count = NLON // 2
    lat_basis = lat_table(NLAT)

    def covariance(residue):
        spectrum = jnp.fft.rfft(residue, axis=-1)[..., :half_count]
        coeffs = jnp.concatenate([jnp.real(spectrum), -jnp.imag(spectrum)], axis=-1)
        mode_values = jnp.einsum('py,ylc->plc', lat_basis, coeffs, precision=lax.Precision.HIGHEST)
        scaled = mode_values * spectral_var[:, None, :]
        grid_coeffs = jnp.einsum('py,plc->ylc', lat_basis, scaled, precision=lax.Precision.HIGHEST)
        cosine_part = grid_coeffs[..., :half_count]
        sine_part = grid_coeffs[..., half_count:]
        nyquist = jnp.zeros_like(cosine_part[..., :1])
        complex_part = lax.complex(jnp.concatenate([cosine_part, nyquist], axis=-1), -jnp.concatenate([sine_part, nyquist], axis=-1))
        return jnp.fft.irfft(complex_part, n=NLON, axis=-1)
    return lax.map(covariance, model_error)
```

```python
import functools

import jax
import jax.numpy as jnp
import ml_dtypes
import numpy as np
from jax import lax
from jax.experimental import pallas as pl
from jax.experimental.pallas import tpu as pltpu
from jax.sharding import PartitionSpec as P

STEPS = 4
LON_REACH = 4
LANES = 128


VMEM = pl.BlockSpec(memory_space=pltpu.VMEM)
SMEM = pl.BlockSpec(memory_space=pltpu.SMEM)


def call(kernel, outs, flops, name, n_in, smem_first=True, scratch=()):
    specs = [SMEM] + [VMEM] * (n_in - 1) if smem_first else [VMEM] * n_in
    return pl.pallas_call(
        kernel,
        out_shape=outs,
        in_specs=specs,
        out_specs=jax.tree.map(lambda _: VMEM, outs),
        scratch_shapes=scratch,
        compiler_params=pltpu.CompilerParams(vmem_limit_bytes=24 * 2**20),
        cost_estimate=pl.CostEstimate(flops=flops, bytes_accessed=0, transcendentals=0),
        name=name,
    )


def f32(*shape):
    return jax.ShapeDtypeStruct(shape, jnp.float32)


def i32(*shape):
    return jax.ShapeDtypeStruct(shape, jnp.int32)


def shifted_tiles(tiles):
    count = len(tiles)
    lane = lax.broadcasted_iota(jnp.int32, tiles[0].shape, tiles[0].ndim - 1)
    axis = tiles[0].ndim - 1

    def at(t, k):
        if k == 0:
            return tiles[t]
        here = pltpu.roll(tiles[t], (-k) % LANES, axis)
        if k > 0:
            beside = pltpu.roll(tiles[(t + 1) % count], (-k) % LANES, axis)
            return jnp.where(lane < LANES - k, here, beside)
        beside = pltpu.roll(tiles[(t - 1) % count], (-k) % LANES, axis)
        return jnp.where(lane >= -k, here, beside)

    return lambda t: [at(t, k) for k in range(-LON_REACH, LON_REACH + 1)]


def tree(values, bits):
    for bit in bits:
        values = [jnp.where(bit, high, low) for low, high in zip(values[::2], values[1::2])]
    return values[0]


def lon_mix(candidates, lon_offset, lon_weight):
    code = lon_offset + LON_REACH
    bits = [(code & 1) != 0, (code & 2) != 0, code >= 4]
    west = tree(candidates[:-1], bits)
    east = tree(candidates[1:], bits)
    return west + lon_weight * (east - west)


def level_step(tiles, load):
    candidates = shifted_tiles(tiles)
    rows = tiles[0].shape[0]
    result = []
    for t in range(len(tiles)):
        cands = candidates(t)
        total = None
        for part, turn in ((0, 0), (1, 1), (2, rows - 1)):
            c, b, a = load(part, t)
            term = a * lon_mix(cands, c, b)
            if turn:
                term = pltpu.roll(term, turn, 0)
            total = term if total is None else total + term
        result.append(total)
    return result


def end_row(ref, top, columns=slice(None)):
    return jnp.where(top, ref[:, ref.shape[1] - 1, columns], ref[:, 0, columns])


def lanes(t):
    return slice(t * LANES, (t + 1) * LANES)


def first_kernel(scalars, v, lat, lon, a, b, out, c3, b3, a3, ce, be, ae):
    levels, rows, width = v.shape
    count = width // LANES

    def one(l, carry):
        for t in range(count):
            sl = lanes(t)
            row = lax.broadcasted_iota(jnp.int32, (rows, LANES), 0)
            off, frac = lat[l, :, sl], a[l, :, sl]
            cc, bb = lon[l, :, sl], b[l, :, sl]
            below = off < 0
            down = jnp.where(below, 1.0 - frac, 0.0)
            here = jnp.where(below, frac, 1.0 - frac)
            up = jnp.where(below, 0.0, frac)
            c3[0, l, :, sl], b3[0, l, :, sl], a3[0, l, :, sl] = cc, bb, here
            c3[1, l, :, sl] = pltpu.roll(cc, rows - 1, 0)
            b3[1, l, :, sl] = pltpu.roll(bb, rows - 1, 0)
            a3[1, l, :, sl] = jnp.where(row == rows - 1, 0.0, pltpu.roll(down, rows - 1, 0))
            c3[2, l, :, sl] = pltpu.roll(cc, 1, 0)
            b3[2, l, :, sl] = pltpu.roll(bb, 1, 0)
            a3[2, l, :, sl] = jnp.where(row == 0, 0.0, pltpu.roll(up, 1, 0))
        tiles = [v[l, :, lanes(t)] for t in range(count)]
        load = lambda part, t: (c3[part, l, :, lanes(t)], b3[part, l, :, lanes(t)], a3[part, l, :, lanes(t)])
        for t, value in enumerate(level_step(tiles, load)):
            out[l, :, lanes(t)] = value
        return carry

    lax.fori_loop(0, levels, one, 0)
    for s in range(2):
        top = scalars[s] == rows - 1
        live = scalars[2 + s].astype(jnp.float32)
        ce[s] = end_row(lon, top)
        be[s] = end_row(b, top)
        off, frac = end_row(lat, top), end_row(a, top)
        below = off < 0
        weight_top = jnp.where(below, 0.0, frac)
        weight_low = jnp.where(below, 1.0 - frac, 0.0)
        ae[s] = jnp.where(top, weight_top, weight_low) * live


def put_edges(full, edges_e, edges_o, top):
    rows = full.shape[1]
    full[:, 0, :] = jnp.where(top, edges_o[...], edges_e[...])
    full[:, rows - 1, :] = jnp.where(top, edges_e[...], edges_o[...])


def next_kernel(scalars, local, edges_e, edges_o, c3, b3, a3, out, full):
    levels, rows, width = local.shape
    count = width // LANES
    full[...] = local[...]
    put_edges(full, edges_e, edges_o, scalars[0] == rows - 1)

    def one(l, carry):
        tiles = [full[l, :, lanes(t)] for t in range(count)]
        load = lambda part, t: (c3[part, l, :, lanes(t)], b3[part, l, :, lanes(t)], a3[part, l, :, lanes(t)])
        for t, value in enumerate(level_step(tiles, load)):
            out[l, :, lanes(t)] = value
        return carry

    lax.fori_loop(0, levels, one, 0)


def edge_kernel(scalars, local, halo_e, halo_o, ce, be, ae, out_e, out_o):
    levels, rows, width = local.shape
    count = width // LANES
    for s, (halo, out) in enumerate(((halo_e, out_e), (halo_o, out_o))):
        tiles = [halo[:, lanes(t)] for t in range(count)]
        candidates = shifted_tiles(tiles)
        for t in range(count):
            own = end_row(local, scalars[s] == rows - 1, lanes(t))
            mixed = lon_mix(candidates(t), ce[s, :, lanes(t)], be[s, :, lanes(t)])
            out[:, lanes(t)] = own + ae[s, :, lanes(t)] * mixed


def rows_kernel(scalars, v, out_e, out_o):
    levels, rows, width = v.shape
    out_e[...] = end_row(v, scalars[0] == rows - 1)
    out_o[...] = end_row(v, scalars[1] == rows - 1)


def halves(x):
    high = x.astype(jnp.bfloat16)
    return high, (x - high.astype(jnp.float32)).astype(jnp.bfloat16)


def split_table(table):
    high = table.astype(ml_dtypes.bfloat16)
    return high, (table - high.astype(np.float64)).astype(ml_dtypes.bfloat16)


def lon_table(lon_count, groups):
    points = np.arange(lon_count)[:, None]
    orders = np.arange(lon_count // 2)[None, :]
    angles = (points * orders % lon_count) * (2.0 * np.pi / lon_count)
    table = np.concatenate([np.cos(angles), np.sin(angles)], axis=1).reshape(lon_count, groups, -1)
    table = np.pad(table, ((0, 0), (0, 0), (0, LANES - table.shape[2])))
    return table.reshape(lon_count, groups * LANES)


def lat_table(lat_count):
    orders = np.arange(lat_count)[:, None]
    points = np.arange(lat_count)[None, :]
    angles = ((2 * points + 1) * orders % (4 * lat_count)) * (np.pi / (2 * lat_count))
    return np.where(orders == 0, np.sqrt(1.0 / lat_count), np.sqrt(2.0 / lat_count)) * np.cos(angles)


def dot(x, y, contract=((1,), (0,))):
    return lax.dot_general(x, y, (contract, ((), ())), preferred_element_type=jnp.float32)


def dot3(x, high, low, contract=((1,), (0,))):
    rows = x.shape[0]
    x_high, x_low = halves(x)
    both = dot(jnp.concatenate([x_high, x_low], axis=0), high, contract)
    return both[:rows] + both[rows:] + dot(x_high, low, contract)


def forward_kernel(columns, scalars, v, local, edges_e, edges_o, table_high, table_low, out, full):
    levels, rows, width = v.shape
    spare = LANES - columns
    hosts = columns // spare
    live = scalars[4].astype(jnp.float32)

    full[...] = local[...]
    put_edges(full, edges_e, edges_o, scalars[0] == rows - 1)
    x = (v[...] - live * full[...]).reshape(levels * rows, width)
    groups = table_high.shape[1] // LANES
    for g in range(0, groups, 2):
        cut = slice(g * LANES, (g + 2) * LANES)
        y = dot3(x, table_high[:, cut], table_low[:, cut])
        for h in range(2):
            part = y[:, lanes(h)].reshape(levels // (hosts + 1), hosts + 1, rows, LANES)
            guest = part[:, hosts]
            lane = lax.broadcasted_iota(jnp.int32, guest.shape, 2)
            for s in range(hosts):
                turned = pltpu.roll(guest, columns - s * spare, 2)
                value = jnp.where(lane < columns, part[:, s], turned)
                for u in range(levels // (hosts + 1)):
                    out[g + h, u * hosts + s] = value[u]


def middle_kernel(x, var, there, back, out):
    groups, tiles, rows, width = x.shape
    hosts = var.shape[0]
    for t in range(0, tiles, 2):
        pair = [i for i in (t, t + 1) if i < tiles]
        block = jnp.concatenate([x[:, i].reshape(groups * rows, width) for i in pair], axis=1)
        scale = jnp.concatenate([var[i % hosts] for i in pair], axis=1)
        high, low = halves(block)
        modes = dot(there[...], jnp.concatenate([high, high, low], axis=0)) * scale
        high, low = halves(modes)
        result = dot(back[...], jnp.concatenate([high, high, low], axis=0))
        for n, i in enumerate(pair):
            out[:, i] = result[:, lanes(n)].reshape(groups, rows, width)


def inverse_kernel(columns, x, table_high, table_low, out, coeffs):
    groups, tiles, rows, width = x.shape
    levels = out.shape[0]
    spare = LANES - columns
    hosts = columns // spare
    for g in range(groups):
        packed = x[g].reshape(tiles // hosts, hosts, rows, width)
        lane = lax.broadcasted_iota(jnp.int32, (tiles // hosts, rows, width), 2)
        guest = packed[:, 0]
        for s in range(hosts):
            turned = pltpu.roll(packed[:, s], (s * spare - columns) % LANES, 2)
            guest = turned if s == 0 else jnp.where(lane >= s * spare, turned, guest)
        for u in range(tiles // hosts):
            for s in range(hosts + 1):
                level = u * (hosts + 1) + s
                value = guest[u] if s == hosts else packed[u, s]
                coeffs[level * rows : (level + 1) * rows, lanes(g)] = value
    y = dot3(coeffs[...], table_high[...], table_low[...], ((1,), (1,)))
    out[...] = y.reshape(out.shape)


def general_spectral(error, var, lat_count, columns, groups):
    lon_count = error.shape[2]
    high = lax.Precision.HIGHEST
    table = jnp.asarray(lon_table(lon_count, groups).reshape(lon_count, groups, LANES)[:, :, :columns], jnp.float32)
    basis = jnp.asarray(lat_table(lat_count), jnp.float32)
    coeffs = jnp.einsum("lyx,xgc->gylc", error, table, precision=high)
    gathered = lax.all_to_all(coeffs, "lat", split_axis=0, concat_axis=0, tiled=True)
    gathered = gathered.reshape(lat_count, error.shape[0], columns)
    modes = jnp.einsum("py,ylc->plc", basis, gathered, precision=high) * var[:, None, :]
    back = jnp.einsum("py,plc->ylc", basis, modes, precision=high)
    back = back.reshape(groups, error.shape[1], error.shape[0], columns)
    back = lax.all_to_all(back, "lat", split_axis=0, concat_axis=0, tiled=True)
    return jnp.einsum("gylc,xgc->lyx", back, table, precision=high)


def partner(lat, parity):
    return lat + 1 if lat % 2 == parity else lat - 1


def pairing(wins, lats, parity):
    pairs = []
    for w in range(wins):
        for l in range(lats):
            other = partner(l, parity)
            if 0 <= other < lats:
                pairs.append((w * lats + l, w * lats + other))
            else:
                pairs.append((w * lats + l, (w ^ 1 if w ^ 1 < wins else w) * lats + l))
    return pairs


def body(perturbation, lat_offset, lon_offset, lat_weight, lon_weight, spectral_var):
    v, lat, lon, a, b = (
        x[0].transpose(1, 0, 2) for x in (perturbation, lat_offset, lon_offset, lat_weight, lon_weight)
    )
    levels, rows, width = v.shape
    wins, lats = lax.axis_size("win"), lax.axis_size("lat")
    win_at, lat_at = lax.axis_index("win"), lax.axis_index("lat")
    lat_count, columns = spectral_var.shape
    groups = width // columns
    even = lat_at % 2 == 0
    row_e = jnp.where(even, rows - 1, 0)
    row_o = jnp.where(even, 0, rows - 1)
    live_e = jnp.where(even, lat_at + 1 < lats, True)
    live_o = jnp.where(even, lat_at > 0, lat_at + 1 < lats)
    scalars = jnp.stack([x.astype(jnp.int32) for x in (row_e, row_o, live_e, live_o, win_at > 0)])
    swaps = [pairing(wins, lats, parity) for parity in (0, 1)]

    orders = (lat_at * columns + jnp.arange(columns)) % (width // 2)
    weights = jnp.where(orders == 0, 1.0, 2.0).astype(jnp.float32) / width
    var = spectral_var * weights[None, :]

    field = f32(levels, rows, width)
    edge = f32(levels, width)
    cost = levels * rows * width * 100
    edges = call(rows_kernel, (edge, edge), 1000, "edge_rows", 2)(scalars, v)
    local = None
    for step in range(STEPS):
        halos = [lax.ppermute(edges[p], ("win", "lat"), swaps[p]) for p in range(2)]
        if step == 0:
            local, c3, b3, a3, ce, be, ae = call(
                first_kernel,
                (field, i32(3, levels, rows, width), f32(3, levels, rows, width), f32(3, levels, rows, width),
                 i32(2, levels, width), f32(2, levels, width), f32(2, levels, width)),
                cost, "first_step", 6,
            )(scalars, v, lat, lon, a, b)
        else:
            local = call(next_kernel, field, cost, "next_step", 7, scratch=[pltpu.VMEM(field.shape, field.dtype)])(
                scalars, local, *edges, c3, b3, a3
            )
        if step == STEPS - 1:
            ring = [(w, (w + 1) % wins) for w in range(wins)]
            moved = lax.ppermute(local, "win", ring)
        edges = call(edge_kernel, (edge, edge), cost // 40, "edge_fix", 7)(scalars, local, *halos, ce, be, ae)
    moved_edges = lax.ppermute(jnp.stack(edges), "win", ring)

    spare = LANES - columns
    packs = 0 < spare < columns and columns % spare == 0 and levels % (columns // spare + 1) == 0 and groups % 2 == 0
    if not packs:
        row = lax.broadcasted_iota(jnp.int32, moved.shape, 1)
        full = jnp.where(row == row_e, moved_edges[0][:, None], jnp.where(row == row_o, moved_edges[1][:, None], moved))
        error = v - jnp.where(win_at > 0, full, 0.0)
        result = general_spectral(error, var, lat_count, columns, groups)
        return result.transpose(1, 0, 2)[None]

    hosts = columns // spare
    tiles = levels // (hosts + 1) * hosts
    table_high, table_low = (jnp.asarray(x) for x in split_table(lon_table(width, groups)))
    packed = f32(groups, tiles, rows, LANES)
    coeffs = pl.pallas_call(
        functools.partial(forward_kernel, columns),
        out_shape=packed,
        in_specs=[SMEM] + [VMEM] * 6,
        out_specs=VMEM,
        scratch_shapes=[pltpu.VMEM((levels, rows, width), jnp.float32)],
        compiler_params=pltpu.CompilerParams(vmem_limit_bytes=24 * 2**20),
        name="forward",
    )(scalars, v, moved, moved_edges[0], moved_edges[1], table_high, table_low)
    gathered = lax.all_to_all(coeffs, "lat", split_axis=0, concat_axis=0, tiled=True)
    scale = jnp.stack([jnp.concatenate([var, var[:, s * spare : (s + 1) * spare]], axis=1) for s in range(hosts)])
    basis_high, basis_low = split_table(lat_table(lat_count))
    back_high, back_low = basis_high.T, basis_low.T
    there = jnp.asarray(np.concatenate([basis_high, basis_low, basis_high], axis=1))
    back = jnp.asarray(np.concatenate([back_high, back_low, back_high], axis=1))
    weighted = call(middle_kernel, packed, 1000, "middle", 4, False)(gathered, scale, there, back)
    returned = lax.all_to_all(weighted, "lat", split_axis=0, concat_axis=0, tiled=True)
    result = pl.pallas_call(
        functools.partial(inverse_kernel, columns),
        out_shape=field,
        in_specs=[VMEM] * 3,
        out_specs=VMEM,
        scratch_shapes=[pltpu.VMEM((levels * rows, groups * LANES), jnp.float32)],
        compiler_params=pltpu.CompilerParams(vmem_limit_bytes=24 * 2**20),
        name="inverse",
    )(returned, table_high, table_low)
    return result.transpose(1, 0, 2)[None]


def solution(mesh):
    in_specs = (
        P("win", "lat", None, None),
        P("win", "lat", None, None),
        P("win", "lat", None, None),
        P("win", "lat", None, None),
        P("win", "lat", None, None),
        P(None, "lat"),
    )
    out_specs = P("win", "lat", None, None)
    return jax.shard_map(body, mesh=mesh, in_specs=in_specs, out_specs=out_specs, check_vma=False)
```
